32 devices in a mesh: fsdp: 8 (over y, x, core), tp: 4 (over z).
Axes of the slice: x: 2, y: 2, z: 4, core: 2. Of those that a mesh axis runs over, the one named last changes fastest.
Arguments:
- w_gate: float32 [3072, 8192], P('fsdp', 'tp'), may hold values from -0.15625 to 0.15625
- first_gate: float32 [3072, 8192], P('fsdp', 'tp'), may hold values from -0.109375 to 0.109375
- second_gate: float32 [3072, 8192], P('fsdp', 'tp'), may hold values from -0.109375 to 0.109375
- w_up: float32 [3072, 8192], P('fsdp', 'tp'), may hold values from -0.15625 to 0.15625
- first_up: float32 [3072, 8192], P('fsdp', 'tp'), may hold values from -0.109375 to 0.109375
- second_up: float32 [3072, 8192], P('fsdp', 'tp'), may hold values from -0.109375 to 0.109375
- norm_train: float32 [3072], P(('fsdp', 'tp')), may hold values from 0.25 to 1.75
- norm_step: float32 [3072], P(('fsdp', 'tp')), may hold values from -0.3 to 0.3
Outputs:
- serving_gate: bfloat16 [3072, 8192], P(None, 'tp')
- serving_up: bfloat16 [3072, 8192], P(None, 'tp')
- scale_gate: float32 [8192], P('tp')
- scale_up: float32 [8192], P('tp')
- serve_norm: bfloat16 [3072], replicated
- whole_gate: float32 [3072, 8192], P('fsdp', 'tp')
- whole_up: float32 [3072, 8192], P('fsdp', 'tp')
The draws below stay inside these ranges and needn't reach their ends.
All inputs are finite; a program needn't handle non-finite values. Where the reference program divides by a largest or mean magnitude, that divisor is 1e-20 or more.
Results may differ from the reference program's by a relative error of at most 0.001.
Values may be sent and summed in bfloat16 or wider, within the bound.
A program may use at most 128 MiB of HBM per device.

```python
import jax
import jax.numpy as jnp

D_MODEL = 3072
D_INNER = 8192


def spiked(entries, rng, source, target, shards_of, factor):
    owner, partner = [(jnp.arange(entries.shape[axis_at]) // (entries.shape[axis_at] // shards_of)).reshape([-1 if axis == axis_at else 1 for axis in range(entries.ndim)]) for axis_at in (source, target)]
    chosen = jax.random.permutation(rng, shards_of)[partner]
    strong = (owner == chosen) | (owner == (partner + shards_of // 2) % shards_of)
    return jnp.where(strong, factor * entries, entries)


def levels(own_key, extent, cuts, least, top_value):
    def one(position, shards_of):
        draws = jax.random.uniform(jax.random.fold_in(jax.random.fold_in(own_key, 6), position), (shards_of,), jnp.float32, least / len(cuts), top_value / len(cuts))
        return jnp.repeat(jnp.exp(draws), extent[position] // shards_of).reshape((-1,) + (1,) * (len(extent) - position - 1))

    loudness = one(*cuts[0])
    for cut in cuts[1:]:
        loudness = loudness * one(*cut)
    return loudness


def noise(rng, dims, width, bound, split=(), held_as=jnp.bfloat16):
    values = width * jax.random.normal(rng, dims, jnp.float32)
    if split:
        values = values * levels(rng, dims, split, -0.22, 0.18)
    return jnp.clip(values, -bound, bound).astype(held_as)


def bell_draw_with(key, shape, deviation, reach, pieces, heavy, dtype=jnp.bfloat16):
    result = deviation * jax.random.normal(key, shape, jnp.float32)
    if pieces:
        result = result * levels(key, shape, pieces, -0.22, 0.18)
    return jnp.clip(spiked(result, jax.random.fold_in(key, 3), *heavy), -reach, reach).astype(dtype)


def setup_inputs(seed: int = 0) -> dict:
    arg_keys = jax.random.split(jax.random.key(seed), 9)
    return {
        "w_gate": bell_draw_with(arg_keys[0], (D_MODEL, D_INNER), D_MODEL ** -0.5, 0.15625, ((0, 8), (1, 4)), (0, 1, 8, 2.0), jnp.float32),
        "first_gate": noise(arg_keys[1], (D_MODEL, D_INNER), D_MODEL ** -0.5, 0.109375, ((0, 8), (1, 4)), jnp.float32),
        "second_gate": noise(arg_keys[2], (D_MODEL, D_INNER), D_MODEL ** -0.5, 0.109375, ((0, 8), (1, 4)), jnp.float32),
        "w_up": bell_draw_with(arg_keys[3], (D_MODEL, D_INNER), D_MODEL ** -0.5, 0.15625, ((0, 8), (1, 4)), (0, 1, 8, 2.0), jnp.float32),
        "first_up": noise(arg_keys[4], (D_MODEL, D_INNER), D_MODEL ** -0.5, 0.109375, ((0, 8), (1, 4)), jnp.float32),
        "second_up": noise(arg_keys[5], (D_MODEL, D_INNER), D_MODEL ** -0.5, 0.109375, ((0, 8), (1, 4)), jnp.float32),
        "norm_train": jnp.clip(1.0 + 0.15 * jax.random.normal(arg_keys[6], (D_MODEL,), jnp.float32), 0.25, 1.75),
        "norm_step": jnp.clip(jax.random.uniform(arg_keys[7], (D_MODEL,), jnp.float32, -0.3, 0.3) * levels(arg_keys[7], (D_MODEL,), ((0, 32),), -0.4, 0.0), -0.3, 0.3),
    }


learn_rate = 0.25
hold_rate = 0.9


def reference(w_gate, first_gate, second_gate, w_up, first_up, second_up, norm_train, norm_step):
    hold_gate = hold_rate * first_gate + second_gate
    whole_gate = w_gate - learn_rate * hold_gate
    hold_up = hold_rate * first_up + second_up
    whole_up = w_up - learn_rate * hold_up
    scale_gate = jnp.sum(jnp.abs(whole_gate), axis=0) / D_MODEL
    serving_gate = (whole_gate / scale_gate).astype(jnp.bfloat16)
    scale_up = jnp.sum(jnp.abs(whole_up), axis=0) / D_MODEL
    serving_up = (whole_up / scale_up).astype(jnp.bfloat16)
    serve_norm = (norm_train + norm_step).astype(jnp.bfloat16)
    return serving_gate, serving_up, scale_gate, scale_up, serve_norm, whole_gate, whole_up
```

```python
import functools

import jax
import jax.numpy as jnp
from jax import lax
from jax.experimental import pallas as pl
from jax.experimental.pallas import tpu as pltpu
from jax.sharding import PartitionSpec as P

LEARN_RATE = 0.25
HOLD_RATE = 0.9
WIDTH = 512
STEP_ROWS = 16


def fused(F, T, R, C, D, S, w_gate, first_gate, second_gate, w_up, first_up, second_up, norm_train, norm_step,
          serving_gate, serving_up, scales, norm_rows, whole_gate, whole_up,
          stage, stats, norm_parts, in_sems, stat_send, stat_recv, part_send, part_recv, row_send, row_recv,
          ring_send, ring_recv, sib_send, sib_recv):
    ins = ((w_gate, first_gate, second_gate), (w_up, first_up, second_up))
    serving = (serving_gate, serving_up)
    whole = (whole_gate, whole_up)
    W = min(WIDTH, C)
    K = C // W
    units = [(m, k) for m in range(2) for k in range(K)]
    U = len(units)
    n = F // 2
    h = n // 2
    Y = n // 2
    me = lax.axis_index("fsdp")
    mt = lax.axis_index("tp")
    chip, core = lax.div(me, 2), lax.rem(me, 2)
    cy, cx = lax.div(chip, 2), lax.rem(chip, 2)
    pos = (1 - cx) * cy + cx * (n - 1 - cy)

    def chip_at(p):
        p = lax.rem(p + n, n)
        flag = lax.div(p, Y)
        return (1 - flag) * (2 * p) + flag * (2 * (n - 1 - p) + 1)

    right = chip_at(pos + 1) * 2 + core
    left = chip_at(pos - 1) * 2 + core
    sib = me + 1 - 2 * core

    def load(u, j):
        m, k = units[u]
        cols = pl.ds(k * W, W)
        return pltpu.make_async_copy(ins[m][j].at[:, cols], stage.at[3 * m + j, :, cols], in_sems.at[3 * u + j])

    for u in range(U):
        for j in range(3):
            load(u, j).start()

    barrier = pltpu.get_barrier_semaphore()
    for d in range(1, F):
        pl.semaphore_signal(barrier, inc=1, device_id={"fsdp": lax.rem(me + d, F)})
    for d in range(1, T):
        pl.semaphore_signal(barrier, inc=1, device_id={"tp": lax.rem(mt + d, T)})

    def unit_stats(u):
        m, k = units[u]
        cols = pl.ds(k * W, W)
        for j in range(3):
            load(u, j).wait()

        def body(i, acc):
            rows = pl.ds(pl.multiple_of(i * STEP_ROWS, STEP_ROWS), STEP_ROWS)
            hold = HOLD_RATE * stage[3 * m + 1, rows, cols] + stage[3 * m + 2, rows, cols]
            new = stage[3 * m, rows, cols] - LEARN_RATE * hold
            whole[m][rows, cols] = new
            mag = jnp.abs(new)
            return acc + mag[:8] + mag[8:]

        acc = lax.fori_loop(0, R // STEP_ROWS, body, jnp.zeros((8, W), jnp.float32))
        stats[me, :, pl.ds(u * W, W)] = jnp.sum(acc, axis=0, keepdims=True)

    def stat_copy(g, d, owner):
        cols = pl.ds(0, W) if g == 0 else pl.ds(W, (U - 1) * W)
        ref = stats.at[owner, :, cols]
        return pltpu.make_async_remote_copy(
            src_ref=ref, dst_ref=ref, send_sem=stat_send.at[g, d], recv_sem=stat_recv.at[g, d],
            device_id={"fsdp": lax.rem(me + d, F)})

    def unit_narrow(u):
        m, k = units[u]
        cols = pl.ds(k * W, W)
        total = stats[0, :, pl.ds(u * W, W)]
        for f in range(1, F):
            total = total + stats[f, :, pl.ds(u * W, W)]
        scale = total / D
        scales[:, pl.ds(u * W, W)] = scale
        inverse = jnp.broadcast_to(1.0 / scale, (STEP_ROWS, W))

        def body(i, carry):
            rows = pl.ds(pl.multiple_of(i * STEP_ROWS, STEP_ROWS), STEP_ROWS)
            to = pl.ds(pl.multiple_of(me * R + i * STEP_ROWS, STEP_ROWS), STEP_ROWS)
            serving[m][to, cols] = (whole[m][rows, cols] * inverse).astype(jnp.bfloat16)
            return carry

        lax.fori_loop(0, R // STEP_ROWS, body, 0)

    def block(u, f, direction, s):
        m, k = units[u]
        start, size = f * R, R
        if s == h:
            size = R // 2
            start = start + direction * size
        return serving[m].at[pl.ds(pl.multiple_of(start, 16), size), pl.ds(k * W, W)]

    def origin(direction, s):
        return chip_at(pos - s) if direction == 0 else chip_at(pos + s)

    def ring_out(u, direction, s):
        ref = block(u, origin(direction, s - 1) * 2 + core, direction, s)
        return pltpu.make_async_remote_copy(
            src_ref=ref, dst_ref=ref, send_sem=ring_send.at[direction, s - 1, u],
            recv_sem=ring_recv.at[direction, s - 1, u], device_id={"fsdp": left if direction else right})

    def ring_in(u, direction, s):
        ref = block(u, origin(direction, s) * 2 + core, direction, s)
        return pltpu.make_async_remote_copy(
            src_ref=ref, dst_ref=ref, send_sem=ring_send.at[direction, s - 1, u],
            recv_sem=ring_recv.at[direction, s - 1, u], device_id={"fsdp": left if direction else right})

    def sib_copy(u, direction, s, at_core):
        if s == 0:
            ref, i = block(u, chip * 2 + at_core, 0, 0), 0
        else:
            ref, i = block(u, origin(direction, s) * 2 + at_core, direction, s), 2 * s - 1 + direction
        return pltpu.make_async_remote_copy(
            src_ref=ref, dst_ref=ref, send_sem=sib_send.at[i, u], recv_sem=sib_recv.at[i, u],
            device_id={"fsdp": sib})

    def part_copy(d, owner):
        ref = norm_parts.at[owner]
        return pltpu.make_async_remote_copy(
            src_ref=ref, dst_ref=ref, send_sem=part_send.at[d], recv_sem=part_recv.at[d],
            device_id={"tp": lax.rem(mt + d, T)})

    def row_copy(d, owner):
        ref = norm_rows.at[owner]
        return pltpu.make_async_remote_copy(
            src_ref=ref, dst_ref=ref, send_sem=row_send.at[d], recv_sem=row_recv.at[d],
            device_id={"fsdp": lax.rem(me + d, F)})

    gain = (norm_train[...] + norm_step[...]).astype(jnp.bfloat16)
    L = norm_rows.shape[-1]
    put = (lax.broadcasted_iota(jnp.int32, (S, L), 1)
           == lax.broadcasted_iota(jnp.int32, (S, L), 0) + mt * S)
    placed = jnp.dot(jnp.broadcast_to(gain, (8, S)), jnp.where(put, 1.0, 0.0).astype(jnp.bfloat16),
                     preferred_element_type=jnp.float32)
    norm_parts[mt] = placed[:1]

    unit_stats(0)
    pl.semaphore_wait(barrier, F - 1 + T - 1)
    for d in range(1, F):
        stat_copy(0, d, me).start()
    for d in range(1, T):
        part_copy(d, mt).start()
    for d in range(1, F):
        stat_copy(0, d, lax.rem(me - d + F, F)).wait_recv()

    def send_own(u):
        for direction in range(2):
            ring_out(u, direction, 1).start()
        sib_copy(u, 0, 0, core).start()

    unit_narrow(0)
    send_own(0)
    for u in range(1, U):
        unit_stats(u)
    for d in range(1, F):
        stat_copy(1, d, me).start()

    for d in range(1, T):
        part_copy(d, lax.rem(mt - d + T, T)).wait_recv()
    row = norm_parts[0]
    for t in range(1, T):
        row = row + norm_parts[t]
    norm_rows[me] = row
    for d in range(1, F):
        row_copy(d, me).start()

    def forward(u, s):
        for direction in range(2):
            ring_in(u, direction, s).wait_recv()
            if s < h:
                ring_out(u, direction, s + 1).start()
            sib_copy(u, direction, s, core).start()

    for d in range(1, F):
        stat_copy(1, d, lax.rem(me - d + F, F)).wait_recv()
    for u in range(1, U):
        unit_narrow(u)
        send_own(u)
    for s in range(1, h + 1):
        for u in range(U):
            forward(u, s)

    for d in range(1, F):
        row_copy(d, lax.rem(me - d + F, F)).wait_recv()
    for u in range(U):
        sib_copy(u, 0, 0, 1 - core).wait_recv()
        sib_copy(u, 0, 0, core).wait_send()
        for s in range(1, h + 1):
            for direction in range(2):
                ring_out(u, direction, s).wait_send()
                sib_copy(u, direction, s, 1 - core).wait_recv()
                sib_copy(u, direction, s, core).wait_send()
    for d in range(1, F):
        stat_copy(0, d, me).wait_send()
        stat_copy(1, d, me).wait_send()
        row_copy(d, me).wait_send()
    for d in range(1, T):
        part_copy(d, mt).wait_send()


def put_out(serving_gate, serving_up, scales, whole_gate, whole_up,
            to_serving_gate, to_serving_up, scale_gate, scale_up, to_whole_gate, to_whole_up, sems):
    copies = [
        pltpu.make_async_copy(source, target, sems.at[i])
        for i, (source, target) in enumerate((
            (serving_gate, to_serving_gate), (serving_up, to_serving_up),
            (whole_gate, to_whole_gate), (whole_up, to_whole_up)))
    ]
    for copy in copies:
        copy.start()
    C = scale_gate.shape[1]
    scale_gate[...] = scales[:, :C]
    scale_up[...] = scales[:, C:]
    for copy in copies:
        copy.wait()


def per_device(F, T, *args):
    R, C = args[0].shape
    S = args[6].shape[0]
    W = min(WIDTH, C)
    U = 2 * (C // W)
    h = F // 4
    L = -(-S * T // 128) * 128
    anywhere = pl.BlockSpec(memory_space=pl.ANY)
    vmem = pl.BlockSpec(memory_space=pltpu.VMEM)
    serving = pltpu.VMEM((R * F, C), jnp.bfloat16)
    whole = pltpu.VMEM((R, C), jnp.float32)
    dma = pltpu.SemaphoreType.DMA
    serving_gate, serving_up, scales, norm_rows, whole_gate, whole_up = pl.pallas_call(
        functools.partial(fused, F, T, R, C, R * F, S),
        out_shape=(serving, serving, pltpu.VMEM((1, 2 * C), jnp.float32), jax.ShapeDtypeStruct((F, 1, L), jnp.float32),
                   whole, whole),
        in_specs=[anywhere] * 6 + [vmem] * 2,
        out_specs=(vmem,) * 6,
        scratch_shapes=[
            pltpu.VMEM((6, R, C), jnp.float32),
            pltpu.VMEM((F, 1, U * W), jnp.float32),
            pltpu.VMEM((T, 1, L), jnp.float32),
            dma((3 * U,)),
            dma((2, F)), dma((2, F)),
            dma((T,)), dma((T,)),
            dma((F,)), dma((F,)),
            dma((2, h, U)), dma((2, h, U)),
            dma((2 * h + 1, U)), dma((2 * h + 1, U)),
        ],
        compiler_params=pltpu.CompilerParams(
            collective_id=0, has_side_effects=True, vmem_limit_bytes=24 * 1024 * 1024),
        name="fused_step",
    )(*args[:6], args[6].reshape(1, S), args[7].reshape(1, S))
    small = jax.ShapeDtypeStruct((1, C), jnp.float32)
    out = pl.pallas_call(
        put_out,
        out_shape=(jax.ShapeDtypeStruct((R * F, C), jnp.bfloat16),) * 2 + (small,) * 2
        + (jax.ShapeDtypeStruct((R, C), jnp.float32),) * 2,
        in_specs=[vmem] * 5,
        out_specs=(anywhere,) * 2 + (vmem,) * 2 + (anywhere,) * 2,
        scratch_shapes=[dma((4,))],
        compiler_params=pltpu.CompilerParams(vmem_limit_bytes=1024 * 1024),
        name="put_out",
    )(serving_gate, serving_up, scales, whole_gate, whole_up)
    serving_gate, serving_up, scale_gate, scale_up, whole_gate, whole_up = out
    serve_norm = norm_rows[:, 0, :S * T].reshape(-1).astype(jnp.bfloat16)
    return (serving_gate, serving_up, scale_gate.reshape(C), scale_up.reshape(C), serve_norm, whole_gate, whole_up)


def solution(mesh):
    F, T = mesh.shape["fsdp"], mesh.shape["tp"]
    return jax.shard_map(
        functools.partial(per_device, F, T),
        mesh=mesh,
        in_specs=(P("fsdp", "tp"),) * 6 + (P(("fsdp", "tp")),) * 2,
        out_specs=(P(None, "tp"), P(None, "tp"), P("tp"), P("tp"), P(), P("fsdp", "tp"), P("fsdp", "tp")),
        check_vma=False,
    )
```

```python
import functools

import jax
import jax.numpy as jnp
from jax import lax
from jax.experimental import pallas as pl
from jax.experimental.pallas import tpu as pltpu
from jax.sharding import PartitionSpec as P

LEARN_RATE = 0.25
HOLD_RATE = 0.9
WIDTH = 512
STEP_ROWS = 16


def fused(F, T, R, C, D, S, w_gate, first_gate, second_gate, w_up, first_up, second_up, norm_train, norm_step,
          *refs):
    pieces = 2 * (C // min(WIDTH, C))
    serving = refs[:pieces]
    (scales, norm_rows, whole_gate, whole_up,
          stage, stats, norm_parts, in_sems, stat_send, stat_recv, part_send, part_recv, row_send, row_recv,
          ring_send, ring_recv, sib_send, sib_recv) = refs[pieces:]
    ins = ((w_gate, first_gate, second_gate), (w_up, first_up, second_up))
    whole = (whole_gate, whole_up)
    W = min(WIDTH, C)
    K = C // W
    units = [(m, k) for m in range(2) for k in range(K)]
    U = len(units)
    n = F // 2
    h = n // 2
    Y = n // 2
    me = lax.axis_index("fsdp")
    mt = lax.axis_index("tp")
    chip, core = lax.div(me, 2), lax.rem(me, 2)
    cy, cx = lax.div(chip, 2), lax.rem(chip, 2)
    pos = (1 - cx) * cy + cx * (n - 1 - cy)

    def chip_at(p):
        p = lax.rem(p + n, n)
        flag = lax.div(p, Y)
        return (1 - flag) * (2 * p) + flag * (2 * (n - 1 - p) + 1)

    right = chip_at(pos + 1) * 2 + core
    left = chip_at(pos - 1) * 2 + core
    sib = me + 1 - 2 * core

    def load(u, j):
        m, k = units[u]
        cols = pl.ds(k * W, W)
        return pltpu.make_async_copy(ins[m][j].at[:, cols], stage.at[3 * m + j, :, cols], in_sems.at[3 * u + j])

    for u in range(U):
        for j in range(3):
            load(u, j).start()

    barrier = pltpu.get_barrier_semaphore()
    for d in range(1, F):
        pl.semaphore_signal(barrier, inc=1, device_id={"fsdp": lax.rem(me + d, F)})
    for d in range(1, T):
        pl.semaphore_signal(barrier, inc=1, device_id={"tp": lax.rem(mt + d, T)})

    def unit_stats(u):
        m, k = units[u]
        cols = pl.ds(k * W, W)
        for j in range(3):
            load(u, j).wait()

        def body(i, acc):
            rows = pl.ds(pl.multiple_of(i * STEP_ROWS, STEP_ROWS), STEP_ROWS)
            hold = HOLD_RATE * stage[3 * m + 1, rows, cols] + stage[3 * m + 2, rows, cols]
            new = stage[3 * m, rows, cols] - LEARN_RATE * hold
            whole[m][rows, cols] = new
            mag = jnp.abs(new)
            return acc + mag[:8] + mag[8:]

        acc = lax.fori_loop(0, R // STEP_ROWS, body, jnp.zeros((8, W), jnp.float32))
        stats[me, :, pl.ds(u * W, W)] = jnp.sum(acc, axis=0, keepdims=True)

    def stat_copy(g, d, owner):
        cols = pl.ds(0, W) if g == 0 else pl.ds(W, (U - 1) * W)
        ref = stats.at[owner, :, cols]
        return pltpu.make_async_remote_copy(
            src_ref=ref, dst_ref=ref, send_sem=stat_send.at[g, d], recv_sem=stat_recv.at[g, d],
            device_id={"fsdp": lax.rem(me + d, F)})

    def unit_narrow(u):
        m, k = units[u]
        cols = pl.ds(k * W, W)
        total = stats[0, :, pl.ds(u * W, W)]
        for f in range(1, F):
            total = total + stats[f, :, pl.ds(u * W, W)]
        scale = total / D
        scales[:, pl.ds(u * W, W)] = scale
        inverse = jnp.broadcast_to(1.0 / scale, (STEP_ROWS, W))

        def body(i, carry):
            rows = pl.ds(pl.multiple_of(i * STEP_ROWS, STEP_ROWS), STEP_ROWS)
            to = pl.ds(pl.multiple_of(me * R + i * STEP_ROWS, STEP_ROWS), STEP_ROWS)
            serving[u][to, :] = (whole[m][rows, cols] * inverse).astype(jnp.bfloat16)
            return carry

        lax.fori_loop(0, R // STEP_ROWS, body, 0)

    def block(u, f, direction, s):
        start, size = f * R, R
        if s == h:
            size = R // 2
            start = start + direction * size
        return serving[u].at[pl.ds(pl.multiple_of(start, 16), size)]

    def origin(direction, s):
        return chip_at(pos - s) if direction == 0 else chip_at(pos + s)

    def ring_out(u, direction, s):
        ref = block(u, origin(direction, s - 1) * 2 + core, direction, s)
        return pltpu.make_async_remote_copy(
            src_ref=ref, dst_ref=ref, send_sem=ring_send.at[direction, s - 1, u],
            recv_sem=ring_recv.at[direction, s - 1, u], device_id={"fsdp": left if direction else right})

    def ring_in(u, direction, s):
        ref = block(u, origin(direction, s) * 2 + core, direction, s)
        return pltpu.make_async_remote_copy(
            src_ref=ref, dst_ref=ref, send_sem=ring_send.at[direction, s - 1, u],
            recv_sem=ring_recv.at[direction, s - 1, u], device_id={"fsdp": left if direction else right})

    def sib_copy(u, direction, s, at_core):
        if s == 0:
            ref, i = block(u, chip * 2 + at_core, 0, 0), 0
        else:
            ref, i = block(u, origin(direction, s) * 2 + at_core, direction, s), 2 * s - 1 + direction
        return pltpu.make_async_remote_copy(
            src_ref=ref, dst_ref=ref, send_sem=sib_send.at[i, u], recv_sem=sib_recv.at[i, u],
            device_id={"fsdp": sib})

    def part_copy(d, owner):
        ref = norm_parts.at[owner]
        return pltpu.make_async_remote_copy(
            src_ref=ref, dst_ref=ref, send_sem=part_send.at[d], recv_sem=part_recv.at[d],
            device_id={"tp": lax.rem(mt + d, T)})

    def row_copy(d, owner):
        ref = norm_rows.at[owner]
        return pltpu.make_async_remote_copy(
            src_ref=ref, dst_ref=ref, send_sem=row_send.at[d], recv_sem=row_recv.at[d],
            device_id={"fsdp": lax.rem(me + d, F)})

    gain = (norm_train[...] + norm_step[...]).astype(jnp.bfloat16)
    L = norm_rows.shape[-1]
    put = (lax.broadcasted_iota(jnp.int32, (S, L), 1)
           == lax.broadcasted_iota(jnp.int32, (S, L), 0) + mt * S)
    placed = jnp.dot(jnp.broadcast_to(gain, (8, S)), jnp.where(put, 1.0, 0.0).astype(jnp.bfloat16),
                     preferred_element_type=jnp.float32)
    norm_parts[mt] = placed[:1]

    unit_stats(0)
    pl.semaphore_wait(barrier, F - 1 + T - 1)
    for d in range(1, F):
        stat_copy(0, d, me).start()
    for d in range(1, T):
        part_copy(d, mt).start()
    for d in range(1, F):
        stat_copy(0, d, lax.rem(me - d + F, F)).wait_recv()

    def send_own(u):
        for direction in range(2):
            ring_out(u, direction, 1).start()
        sib_copy(u, 0, 0, core).start()

    unit_narrow(0)
    send_own(0)
    for u in range(1, U):
        unit_stats(u)
    for d in range(1, F):
        stat_copy(1, d, me).start()

    for d in range(1, T):
        part_copy(d, lax.rem(mt - d + T, T)).wait_recv()
    row = norm_parts[0]
    for t in range(1, T):
        row = row + norm_parts[t]
    norm_rows[me] = row
    for d in range(1, F):
        row_copy(d, me).start()

    def forward(u, s):
        for direction in range(2):
            ring_in(u, direction, s).wait_recv()
            if s < h:
                ring_out(u, direction, s + 1).start()
            sib_copy(u, direction, s, core).start()

    for d in range(1, F):
        stat_copy(1, d, lax.rem(me - d + F, F)).wait_recv()
    for u in range(1, U):
        unit_narrow(u)
        send_own(u)
    for s in range(1, h + 1):
        for u in range(U):
            forward(u, s)

    for d in range(1, F):
        row_copy(d, lax.rem(me - d + F, F)).wait_recv()
    for u in range(U):
        sib_copy(u, 0, 0, 1 - core).wait_recv()
        sib_copy(u, 0, 0, core).wait_send()
        for s in range(1, h + 1):
            for direction in range(2):
                ring_out(u, direction, s).wait_send()
                sib_copy(u, direction, s, 1 - core).wait_recv()
                sib_copy(u, direction, s, core).wait_send()
    for d in range(1, F):
        stat_copy(0, d, me).wait_send()
        stat_copy(1, d, me).wait_send()
        row_copy(d, me).wait_send()
    for d in range(1, T):
        part_copy(d, mt).wait_send()


def put_out(*refs):
    serving = refs[:-12]
    (scales, norm_rows, whole_gate, whole_up, to_serving_gate, to_serving_up, scale_gate, scale_up, serve_norm,
     to_whole_gate, to_whole_up, sems) = refs[-12:]
    W = serving[0].shape[1]
    K = len(serving) // 2
    pairs = [(piece, (to_serving_gate, to_serving_up)[u // K].at[:, pl.ds(u % K * W, W)])
             for u, piece in enumerate(serving)]
    pairs += [(whole_gate, to_whole_gate), (whole_up, to_whole_up)]
    copies = [pltpu.make_async_copy(source, target, sems.at[i]) for i, (source, target) in enumerate(pairs)]
    for copy in copies:
        copy.start()
    C = scale_gate.shape[1]
    scale_gate[...] = scales[:, :C]
    scale_up[...] = scales[:, C:]
    F, _, L = norm_rows.shape
    for f in range(F):
        serve_norm[:, pl.ds(f * L, L)] = norm_rows[f].astype(jnp.bfloat16)
    for copy in copies:
        copy.wait()


def per_device(F, T, *args):
    R, C = args[0].shape
    S = args[6].shape[0]
    W = min(WIDTH, C)
    U = 2 * (C // W)
    h = F // 4
    L = -(-S * T // 128) * 128
    anywhere = pl.BlockSpec(memory_space=pl.ANY)
    vmem = pl.BlockSpec(memory_space=pltpu.VMEM)
    piece = pltpu.VMEM((R * F, W), jnp.bfloat16)
    whole = pltpu.VMEM((R, C), jnp.float32)
    dma = pltpu.SemaphoreType.DMA
    held = pl.pallas_call(
        functools.partial(fused, F, T, R, C, R * F, S),
        out_shape=(piece,) * U + (pltpu.VMEM((1, 2 * C), jnp.float32), pltpu.VMEM((F, 1, L), jnp.float32),
                   whole, whole),
        in_specs=[anywhere] * 6 + [vmem] * 2,
        out_specs=(vmem,) * (U + 4),
        scratch_shapes=[
            pltpu.VMEM((6, R, C), jnp.float32),
            pltpu.VMEM((F, 1, U * W), jnp.float32),
            pltpu.VMEM((T, 1, L), jnp.float32),
            dma((3 * U,)),
            dma((2, F)), dma((2, F)),
            dma((T,)), dma((T,)),
            dma((F,)), dma((F,)),
            dma((2, h, U)), dma((2, h, U)),
            dma((2 * h + 1, U)), dma((2 * h + 1, U)),
        ],
        compiler_params=pltpu.CompilerParams(
            collective_id=0, has_side_effects=True, vmem_limit_bytes=24 * 1024 * 1024),
        name="fused_step",
    )(*args[:6], args[6].reshape(1, S), args[7].reshape(1, S))
    small = jax.ShapeDtypeStruct((1, C), jnp.float32)
    out = pl.pallas_call(
        put_out,
        out_shape=(jax.ShapeDtypeStruct((R * F, C), jnp.bfloat16),) * 2 + (small,) * 2
        + (jax.ShapeDtypeStruct((1, F * L), jnp.bfloat16),) + (jax.ShapeDtypeStruct((R, C), jnp.float32),) * 2,
        in_specs=[vmem] * (U + 4),
        out_specs=(anywhere,) * 2 + (vmem,) * 3 + (anywhere,) * 2,
        scratch_shapes=[dma((U + 2,))],
        compiler_params=pltpu.CompilerParams(vmem_limit_bytes=1024 * 1024),
        name="put_out",
    )(*held)
    serving_gate, serving_up, scale_gate, scale_up, serve_norm, whole_gate, whole_up = out
    serve_norm = serve_norm.reshape(F, L)[:, :S * T].reshape(-1)
    return (serving_gate, serving_up, scale_gate.reshape(C), scale_up.reshape(C), serve_norm, whole_gate, whole_up)


def solution(mesh):
    F, T = mesh.shape["fsdp"], mesh.shape["tp"]
    return jax.shard_map(
        functools.partial(per_device, F, T),
        mesh=mesh,
        in_specs=(P("fsdp", "tp"),) * 6 + (P(("fsdp", "tp")),) * 2,
        out_specs=(P(None, "tp"), P(None, "tp"), P("tp"), P("tp"), P(), P("fsdp", "tp"), P("fsdp", "tp")),
        check_vma=False,
    )
```

```python
import functools

import jax
import jax.numpy as jnp
from jax import lax
from jax.experimental import pallas as pl
from jax.experimental.pallas import tpu as pltpu
from jax.sharding import PartitionSpec as P

LEARN_RATE = 0.25
HOLD_RATE = 0.9
WIDTH = 512
STEP_ROWS = 16


def fused(F, T, R, C, D, S, w_gate, first_gate, second_gate, w_up, first_up, second_up, norm_train, norm_step,
          *refs):
    pieces = 2 * (C // min(WIDTH, C))
    serving = refs[:pieces]
    (scales, norm_rows, whole_gate, whole_up,
          stage, stats, norm_parts, in_sems, stat_send, stat_recv, part_send, part_recv, row_send, row_recv,
          ring_send, ring_recv, sib_send, sib_recv) = refs[pieces:]
    ins = ((w_gate, first_gate, second_gate), (w_up, first_up, second_up))
    whole = (whole_gate, whole_up)
    W = min(WIDTH, C)
    K = C // W
    units = [(m, k) for m in range(2) for k in range(K)]
    U = len(units)
    n = F // 2
    h = n // 2
    Y = n // 2
    me = lax.axis_index("fsdp")
    mt = lax.axis_index("tp")
    chip, core = lax.div(me, 2), lax.rem(me, 2)
    cy, cx = lax.div(chip, 2), lax.rem(chip, 2)
    pos = (1 - cx) * cy + cx * (n - 1 - cy)

    def chip_at(p):
        p = lax.rem(p + n, n)
        flag = lax.div(p, Y)
        return (1 - flag) * (2 * p) + flag * (2 * (n - 1 - p) + 1)

    right = chip_at(pos + 1) * 2 + core
    left = chip_at(pos - 1) * 2 + core
    sib = me + 1 - 2 * core

    def load(u, j):
        m, k = units[u]
        cols = pl.ds(k * W, W)
        return pltpu.make_async_copy(ins[m][j].at[:, cols], stage.at[3 * m + j, :, cols], in_sems.at[3 * u + j])

    for j in range(3):
        load(0, j).start()

    barrier = pltpu.get_barrier_semaphore()
    for d in range(1, F):
        pl.semaphore_signal(barrier, inc=1, device_id={"fsdp": lax.rem(me + d, F)})
    for d in range(1, T):
        pl.semaphore_signal(barrier, inc=1, device_id={"tp": lax.rem(mt + d, T)})

    def unit_stats(u):
        m, k = units[u]
        cols = pl.ds(k * W, W)
        for j in range(3):
            load(u, j).wait()
        if u == 0:
            for later in range(1, U):
                for j in range(3):
                    load(later, j).start()

        def body(i, acc):
            rows = pl.ds(pl.multiple_of(i * STEP_ROWS, STEP_ROWS), STEP_ROWS)
            hold = HOLD_RATE * stage[3 * m + 1, rows, cols] + stage[3 * m + 2, rows, cols]
            new = stage[3 * m, rows, cols] - LEARN_RATE * hold
            whole[m][rows, cols] = new
            mag = jnp.abs(new)
            return acc + mag[:8] + mag[8:]

        acc = lax.fori_loop(0, R // STEP_ROWS, body, jnp.zeros((8, W), jnp.float32))
        stats[me, :, pl.ds(u * W, W)] = jnp.sum(acc, axis=0, keepdims=True)

    def stat_copy(g, d, owner):
        cols = pl.ds(0, W) if g == 0 else pl.ds(W, (U - 1) * W)
        ref = stats.at[owner, :, cols]
        return pltpu.make_async_remote_copy(
            src_ref=ref, dst_ref=ref, send_sem=stat_send.at[g, d], recv_sem=stat_recv.at[g, d],
            device_id={"fsdp": lax.rem(me + d, F)})

    def unit_narrow(u):
        m, k = units[u]
        cols = pl.ds(k * W, W)
        total = stats[0, :, pl.ds(u * W, W)]
        for f in range(1, F):
            total = total + stats[f, :, pl.ds(u * W, W)]
        scale = total / D
        scales[:, pl.ds(u * W, W)] = scale
        inverse = jnp.broadcast_to(1.0 / scale, (STEP_ROWS, W))

        def body(i, carry):
            rows = pl.ds(pl.multiple_of(i * STEP_ROWS, STEP_ROWS), STEP_ROWS)
            to = pl.ds(pl.multiple_of(me * R + i * STEP_ROWS, STEP_ROWS), STEP_ROWS)
            serving[u][to, :] = (whole[m][rows, cols] * inverse).astype(jnp.bfloat16)
            return carry

        lax.fori_loop(0, R // STEP_ROWS, body, 0)

    def block(u, f, part):
        start, size = f * R, R
        if part < 2:
            size = R // 2
            start = start + part * size
        return serving[u].at[pl.ds(pl.multiple_of(start, 16), size)]

    def parts(u, direction, s):
        if s == h:
            return [direction]
        return [direction, 1 - direction] if u == 0 else [2]

    def origin(direction, s):
        return chip_at(pos - s) if direction == 0 else chip_at(pos + s)

    def ring_copy(u, direction, s, part, back):
        ref = block(u, origin(direction, back) * 2 + core, part)
        return pltpu.make_async_remote_copy(
            src_ref=ref, dst_ref=ref, send_sem=ring_send.at[direction, s - 1, part, u],
            recv_sem=ring_recv.at[direction, s - 1, part, u], device_id={"fsdp": left if direction else right})

    def ring_out(u, direction, s, part):
        return ring_copy(u, direction, s, part, s - 1)

    def ring_in(u, direction, s, part):
        return ring_copy(u, direction, s, part, s)

    def sib_copy(u, direction, s, part, at_core):
        ref = block(u, origin(direction, s) * 2 + at_core, part)
        i = 0 if s == 0 else 2 * s - 1 + direction
        return pltpu.make_async_remote_copy(
            src_ref=ref, dst_ref=ref, send_sem=sib_send.at[i, part, u], recv_sem=sib_recv.at[i, part, u],
            device_id={"fsdp": sib})

    def part_copy(d, owner):
        ref = norm_parts.at[owner]
        return pltpu.make_async_remote_copy(
            src_ref=ref, dst_ref=ref, send_sem=part_send.at[d], recv_sem=part_recv.at[d],
            device_id={"tp": lax.rem(mt + d, T)})

    def row_copy(d, owner):
        ref = norm_rows.at[owner]
        return pltpu.make_async_remote_copy(
            src_ref=ref, dst_ref=ref, send_sem=row_send.at[d], recv_sem=row_recv.at[d],
            device_id={"fsdp": lax.rem(me + d, F)})

    gain = (norm_train[...] + norm_step[...]).astype(jnp.bfloat16)
    L = norm_rows.shape[-1]
    put = (lax.broadcasted_iota(jnp.int32, (S, L), 1)
           == lax.broadcasted_iota(jnp.int32, (S, L), 0) + mt * S)
    placed = jnp.dot(jnp.broadcast_to(gain, (8, S)), jnp.where(put, 1.0, 0.0).astype(jnp.bfloat16),
                     preferred_element_type=jnp.float32)
    norm_parts[mt] = placed[:1]

    unit_stats(0)
    pl.semaphore_wait(barrier, F - 1 + T - 1)
    for d in range(1, F):
        stat_copy(0, d, me).start()
    for d in range(1, T):
        part_copy(d, mt).start()
    for d in range(1, F):
        stat_copy(0, d, lax.rem(me - d + F, F)).wait_recv()

    def send_own(u):
        for i in range(len(parts(u, 0, 1))):
            for direction in range(2):
                ring_out(u, direction, 1, parts(u, direction, 1)[i]).start()
        sib_copy(u, 0, 0, 2, core).start()

    unit_narrow(0)
    send_own(0)
    for u in range(1, U):
        unit_stats(u)
    for d in range(1, F):
        stat_copy(1, d, me).start()

    for d in range(1, T):
        part_copy(d, lax.rem(mt - d + T, T)).wait_recv()
    row = norm_parts[0]
    for t in range(1, T):
        row = row + norm_parts[t]
    norm_rows[me] = row
    for d in range(1, F):
        row_copy(d, me).start()

    def forward(u, s, i):
        for direction in range(2):
            part = parts(u, direction, s)[i]
            ring_in(u, direction, s, part).wait_recv()
            if s + 1 < h:
                ring_out(u, direction, s + 1, part).start()
            elif s < h and part in (2, direction):
                ring_out(u, direction, h, direction).start()
            sib_copy(u, direction, s, part, core).start()

    early = [(0, 1, 0)] if h > 1 else []
    for which in early:
        forward(*which)

    for d in range(1, F):
        stat_copy(1, d, lax.rem(me - d + F, F)).wait_recv()
    for u in range(1, U):
        unit_narrow(u)
        send_own(u)
    for s in range(1, h + 1):
        for u in range(U):
            for i in range(len(parts(u, 0, s))):
                if (u, s, i) not in early:
                    forward(u, s, i)

    for d in range(1, F):
        row_copy(d, lax.rem(me - d + F, F)).wait_recv()
    for u in range(U):
        sib_copy(u, 0, 0, 2, 1 - core).wait_recv()
        sib_copy(u, 0, 0, 2, core).wait_send()
        for s in range(1, h + 1):
            for direction in range(2):
                for part in parts(u, direction, s):
                    ring_out(u, direction, s, part).wait_send()
                    sib_copy(u, direction, s, part, 1 - core).wait_recv()
                    sib_copy(u, direction, s, part, core).wait_send()
    for d in range(1, F):
        stat_copy(0, d, me).wait_send()
        stat_copy(1, d, me).wait_send()
        row_copy(d, me).wait_send()
    for d in range(1, T):
        part_copy(d, mt).wait_send()


def put_out(*refs):
    serving = refs[:-12]
    (scales, norm_rows, whole_gate, whole_up, to_serving_gate, to_serving_up, scale_gate, scale_up, serve_norm,
     to_whole_gate, to_whole_up, sems) = refs[-12:]
    W = serving[0].shape[1]
    K = len(serving) // 2
    pairs = [(piece, (to_serving_gate, to_serving_up)[u // K].at[:, pl.ds(u % K * W, W)])
             for u, piece in enumerate(serving)]
    pairs += [(whole_gate, to_whole_gate), (whole_up, to_whole_up)]
    copies = [pltpu.make_async_copy(source, target, sems.at[i]) for i, (source, target) in enumerate(pairs)]
    for copy in copies:
        copy.start()
    C = scale_gate.shape[1]
    scale_gate[...] = scales[:, :C]
    scale_up[...] = scales[:, C:]
    F, _, L = norm_rows.shape
    for f in range(F):
        serve_norm[pl.ds(f * L, L)] = norm_rows[f, 0].astype(jnp.bfloat16)
    for copy in copies:
        copy.wait()


def per_device(F, T, *args):
    R, C = args[0].shape
    S = args[6].shape[0]
    W = min(WIDTH, C)
    U = 2 * (C // W)
    h = F // 4
    L = -(-S * T // 128) * 128
    anywhere = pl.BlockSpec(memory_space=pl.ANY)
    vmem = pl.BlockSpec(memory_space=pltpu.VMEM)
    piece = pltpu.VMEM((R * F, W), jnp.bfloat16)
    whole = pltpu.VMEM((R, C), jnp.float32)
    dma = pltpu.SemaphoreType.DMA
    held = pl.pallas_call(
        functools.partial(fused, F, T, R, C, R * F, S),
        out_shape=(piece,) * U + (pltpu.VMEM((1, 2 * C), jnp.float32), pltpu.VMEM((F, 1, L), jnp.float32),
                   whole, whole),
        in_specs=[anywhere] * 6 + [vmem] * 2,
        out_specs=(vmem,) * (U + 4),
        scratch_shapes=[
            pltpu.VMEM((6, R, C), jnp.float32),
            pltpu.VMEM((F, 1, U * W), jnp.float32),
            pltpu.VMEM((T, 1, L), jnp.float32),
            dma((3 * U,)),
            dma((2, F)), dma((2, F)),
            dma((T,)), dma((T,)),
            dma((F,)), dma((F,)),
            dma((2, h, 3, U)), dma((2, h, 3, U)),
            dma((2 * h + 1, 3, U)), dma((2 * h + 1, 3, U)),
        ],
        compiler_params=pltpu.CompilerParams(
            collective_id=0, has_side_effects=True, vmem_limit_bytes=24 * 1024 * 1024),
        name="fused_step",
    )(*args[:6], args[6].reshape(1, S), args[7].reshape(1, S))
    small = jax.ShapeDtypeStruct((1, C), jnp.float32)
    out = pl.pallas_call(
        put_out,
        out_shape=(jax.ShapeDtypeStruct((R * F, C), jnp.bfloat16),) * 2 + (small,) * 2
        + (jax.ShapeDtypeStruct((F * L,), jnp.bfloat16),) + (jax.ShapeDtypeStruct((R, C), jnp.float32),) * 2,
        in_specs=[vmem] * (U + 4),
        out_specs=(anywhere,) * 2 + (vmem,) * 3 + (anywhere,) * 2,
        scratch_shapes=[dma((U + 2,))],
        compiler_params=pltpu.CompilerParams(vmem_limit_bytes=1024 * 1024),
        name="put_out",
    )(*held)
    serving_gate, serving_up, scale_gate, scale_up, serve_norm, whole_gate, whole_up = out
    if L > S * T:
        serve_norm = serve_norm.reshape(F, L)[:, :S * T].reshape(-1)
    return (serving_gate, serving_up, scale_gate.reshape(C), scale_up.reshape(C), serve_norm, whole_gate, whole_up)


def solution(mesh):
    F, T = mesh.shape["fsdp"], mesh.shape["tp"]
    return jax.shard_map(
        functools.partial(per_device, F, T),
        mesh=mesh,
        in_specs=(P("fsdp", "tp"),) * 6 + (P(("fsdp", "tp")),) * 2,
        out_specs=(P(None, "tp"), P(None, "tp"), P("tp"), P("tp"), P(), P("fsdp", "tp"), P("fsdp", "tp")),
        check_vma=False,
    )
```

```python
import functools

import jax
import jax.numpy as jnp
from jax import lax
from jax.experimental import pallas as pl
from jax.experimental.pallas import tpu as pltpu
from jax.sharding import PartitionSpec as P

LEARN_RATE = 0.25
HOLD_RATE = 0.9
STEP_ROWS = 16


def units_of(C):
    q = C // 4
    return [(0, 0, q), (0, q, q), (0, 2 * q, 2 * q), (1, 0, 2 * q), (1, 2 * q, q), (1, 3 * q, q)]


def fused(F, T, R, C, D, S, w_gate, first_gate, second_gate, w_up, first_up, second_up, norm_train, norm_step,
          *refs):
    pieces = len(units_of(C))
    serving = refs[:pieces]
    (scales, norm_rows, whole_gate, whole_up,
          stage, stats, norm_parts, in_sems, stat_send, stat_recv, part_send, part_recv, row_send, row_recv,
          ring_send, ring_recv, sib_send, sib_recv) = refs[pieces:]
    ins = ((w_gate, first_gate, second_gate), (w_up, first_up, second_up))
    whole = (whole_gate, whole_up)
    units = units_of(C)
    U = len(units)
    first = units[0][2]
    n = F // 2
    h = n // 2
    Y = n // 2
    me = lax.axis_index("fsdp")
    mt = lax.axis_index("tp")
    chip, core = lax.div(me, 2), lax.rem(me, 2)
    cy, cx = lax.div(chip, 2), lax.rem(chip, 2)
    pos = (1 - cx) * cy + cx * (n - 1 - cy)

    def chip_at(p):
        p = lax.rem(p + n, n)
        flag = lax.div(p, Y)
        return (1 - flag) * (2 * p) + flag * (2 * (n - 1 - p) + 1)

    right = chip_at(pos + 1) * 2 + core
    left = chip_at(pos - 1) * 2 + core
    sib = me + 1 - 2 * core

    def load(u, j):
        m, k, W = units[u]
        cols = pl.ds(k, W)
        return pltpu.make_async_copy(ins[m][j].at[:, cols], stage.at[3 * m + j, :, cols], in_sems.at[3 * u + j])

    for j in range(3):
        load(0, j).start()

    barrier = pltpu.get_barrier_semaphore()
    for d in range(1, F):
        pl.semaphore_signal(barrier, inc=1, device_id={"fsdp": lax.rem(me + d, F)})
    for d in range(1, T):
        pl.semaphore_signal(barrier, inc=1, device_id={"tp": lax.rem(mt + d, T)})

    def unit_stats(u):
        m, k, W = units[u]
        cols = pl.ds(k, W)
        for j in range(3):
            load(u, j).wait()
        if u == 0:
            for later in range(1, U):
                for j in range(3):
                    load(later, j).start()

        def body(i, acc):
            rows = pl.ds(pl.multiple_of(i * STEP_ROWS, STEP_ROWS), STEP_ROWS)
            hold = HOLD_RATE * stage[3 * m + 1, rows, cols] + stage[3 * m + 2, rows, cols]
            new = stage[3 * m, rows, cols] - LEARN_RATE * hold
            whole[m][rows, cols] = new
            mag = jnp.abs(new)
            return acc + mag[:8] + mag[8:]

        acc = lax.fori_loop(0, R // STEP_ROWS, body, jnp.zeros((8, W), jnp.float32))
        stats[me, :, pl.ds(m * C + k, W)] = jnp.sum(acc, axis=0, keepdims=True)

    def stat_copy(g, d, owner):
        cols = pl.ds(0, first) if g == 0 else pl.ds(first, 2 * C - first)
        ref = stats.at[owner, :, cols]
        return pltpu.make_async_remote_copy(
            src_ref=ref, dst_ref=ref, send_sem=stat_send.at[g, d], recv_sem=stat_recv.at[g, d],
            device_id={"fsdp": lax.rem(me + d, F)})

    def unit_narrow(u):
        m, k, W = units[u]
        cols = pl.ds(k, W)
        total = stats[0, :, pl.ds(m * C + k, W)]
        for f in range(1, F):
            total = total + stats[f, :, pl.ds(m * C + k, W)]
        scale = total / D
        scales[:, pl.ds(m * C + k, W)] = scale
        inverse = jnp.broadcast_to(1.0 / scale, (STEP_ROWS, W))

        def body(i, carry):
            rows = pl.ds(pl.multiple_of(i * STEP_ROWS, STEP_ROWS), STEP_ROWS)
            to = pl.ds(pl.multiple_of(me * R + i * STEP_ROWS, STEP_ROWS), STEP_ROWS)
            serving[u][to, :] = (whole[m][rows, cols] * inverse).astype(jnp.bfloat16)
            return carry

        lax.fori_loop(0, R // STEP_ROWS, body, 0)

    def block(u, f, part):
        start, size = f * R, R
        if part < 2:
            size = R // 2
            start = start + part * size
        return serving[u].at[pl.ds(pl.multiple_of(start, 16), size)]

    def parts(u, direction, s):
        if s == h:
            return [direction]
        return [direction, 1 - direction] if u == 0 else [2]

    def origin(direction, s):
        return chip_at(pos - s) if direction == 0 else chip_at(pos + s)

    def ring_copy(u, direction, s, part, back):
        ref = block(u, origin(direction, back) * 2 + core, part)
        return pltpu.make_async_remote_copy(
            src_ref=ref, dst_ref=ref, send_sem=ring_send.at[direction, s - 1, part, u],
            recv_sem=ring_recv.at[direction, s - 1, part, u], device_id={"fsdp": left if direction else right})

    def ring_out(u, direction, s, part):
        return ring_copy(u, direction, s, part, s - 1)

    def ring_in(u, direction, s, part):
        return ring_copy(u, direction, s, part, s)

    def sib_copy(u, direction, s, part, at_core):
        ref = block(u, origin(direction, s) * 2 + at_core, part)
        i = 0 if s == 0 else 2 * s - 1 + direction
        return pltpu.make_async_remote_copy(
            src_ref=ref, dst_ref=ref, send_sem=sib_send.at[i, part, u], recv_sem=sib_recv.at[i, part, u],
            device_id={"fsdp": sib})

    def part_copy(d, owner):
        ref = norm_parts.at[owner]
        return pltpu.make_async_remote_copy(
            src_ref=ref, dst_ref=ref, send_sem=part_send.at[d], recv_sem=part_recv.at[d],
            device_id={"tp": lax.rem(mt + d, T)})

    def row_copy(d, owner):
        ref = norm_rows.at[owner]
        return pltpu.make_async_remote_copy(
            src_ref=ref, dst_ref=ref, send_sem=row_send.at[d], recv_sem=row_recv.at[d],
            device_id={"fsdp": lax.rem(me + d, F)})

    gain = (norm_train[...] + norm_step[...]).astype(jnp.bfloat16)
    L = norm_rows.shape[-1]
    put = (lax.broadcasted_iota(jnp.int32, (S, L), 1)
           == lax.broadcasted_iota(jnp.int32, (S, L), 0) + mt * S)
    placed = jnp.dot(jnp.broadcast_to(gain, (8, S)), jnp.where(put, 1.0, 0.0).astype(jnp.bfloat16),
                     preferred_element_type=jnp.float32)
    norm_parts[mt] = placed[:1]

    unit_stats(0)
    pl.semaphore_wait(barrier, F - 1 + T - 1)
    for d in range(1, F):
        stat_copy(0, d, me).start()
    for d in range(1, T):
        part_copy(d, mt).start()
    for d in range(1, F):
        stat_copy(0, d, lax.rem(me - d + F, F)).wait_recv()

    def send_own(u):
        for i in range(len(parts(u, 0, 1))):
            for direction in range(2):
                ring_out(u, direction, 1, parts(u, direction, 1)[i]).start()
        sib_copy(u, 0, 0, 2, core).start()

    unit_narrow(0)
    send_own(0)
    for u in range(1, U):
        unit_stats(u)
    for d in range(1, F):
        stat_copy(1, d, me).start()

    for d in range(1, T):
        part_copy(d, lax.rem(mt - d + T, T)).wait_recv()
    row = norm_parts[0]
    for t in range(1, T):
        row = row + norm_parts[t]
    norm_rows[me] = row
    for d in range(1, F):
        row_copy(d, me).start()

    def forward(u, s, i):
        for direction in range(2):
            part = parts(u, direction, s)[i]
            ring_in(u, direction, s, part).wait_recv()
            if s + 1 < h:
                ring_out(u, direction, s + 1, part).start()
            elif s < h and part in (2, direction):
                ring_out(u, direction, h, direction).start()
            sib_copy(u, direction, s, part, core).start()

    early = [(0, 1, 0)] if h > 1 else []
    for which in early:
        forward(*which)

    for d in range(1, F):
        stat_copy(1, d, lax.rem(me - d + F, F)).wait_recv()
    for u in range(1, U):
        unit_narrow(u)
        send_own(u)
    for s in range(1, h + 1):
        for u in range(U):
            for i in range(len(parts(u, 0, s))):
                if (u, s, i) not in early:
                    forward(u, s, i)

    for d in range(1, F):
        row_copy(d, lax.rem(me - d + F, F)).wait_recv()
    for u in range(U):
        sib_copy(u, 0, 0, 2, 1 - core).wait_recv()
        sib_copy(u, 0, 0, 2, core).wait_send()
        for s in range(1, h + 1):
            for direction in range(2):
                for part in parts(u, direction, s):
                    ring_out(u, direction, s, part).wait_send()
                    sib_copy(u, direction, s, part, 1 - core).wait_recv()
                    sib_copy(u, direction, s, part, core).wait_send()
    for d in range(1, F):
        stat_copy(0, d, me).wait_send()
        stat_copy(1, d, me).wait_send()
        row_copy(d, me).wait_send()
    for d in range(1, T):
        part_copy(d, mt).wait_send()


def put_out(*refs):
    serving = refs[:-12]
    (scales, norm_rows, whole_gate, whole_up, to_serving_gate, to_serving_up, scale_gate, scale_up, serve_norm,
     to_whole_gate, to_whole_up, sems) = refs[-12:]
    pairs = [(piece, (to_serving_gate, to_serving_up)[m].at[:, pl.ds(k, W)])
             for piece, (m, k, W) in zip(serving, units_of(to_serving_gate.shape[1]))]
    pairs += [(whole_gate, to_whole_gate), (whole_up, to_whole_up)]
    copies = [pltpu.make_async_copy(source, target, sems.at[i]) for i, (source, target) in enumerate(pairs)]
    for copy in copies:
        copy.start()
    C = scale_gate.shape[1]
    scale_gate[...] = scales[:, :C]
    scale_up[...] = scales[:, C:]
    F, _, L = norm_rows.shape
    for f in range(F):
        serve_norm[pl.ds(f * L, L)] = norm_rows[f, 0].astype(jnp.bfloat16)
    for copy in copies:
        copy.wait()


def per_device(F, T, *args):
    R, C = args[0].shape
    S = args[6].shape[0]
    units = units_of(C)
    U = len(units)
    h = F // 4
    L = -(-S * T // 128) * 128
    anywhere = pl.BlockSpec(memory_space=pl.ANY)
    vmem = pl.BlockSpec(memory_space=pltpu.VMEM)
    pieces = tuple(pltpu.VMEM((R * F, W), jnp.bfloat16) for _, _, W in units)
    whole = pltpu.VMEM((R, C), jnp.float32)
    dma = pltpu.SemaphoreType.DMA
    held = pl.pallas_call(
        functools.partial(fused, F, T, R, C, R * F, S),
        out_shape=pieces + (pltpu.VMEM((1, 2 * C), jnp.float32), pltpu.VMEM((F, 1, L), jnp.float32),
                   whole, whole),
        in_specs=[anywhere] * 6 + [vmem] * 2,
        out_specs=(vmem,) * (U + 4),
        scratch_shapes=[
            pltpu.VMEM((6, R, C), jnp.float32),
            pltpu.VMEM((F, 1, 2 * C), jnp.float32),
            pltpu.VMEM((T, 1, L), jnp.float32),
            dma((3 * U,)),
            dma((2, F)), dma((2, F)),
            dma((T,)), dma((T,)),
            dma((F,)), dma((F,)),
            dma((2, h, 3, U)), dma((2, h, 3, U)),
            dma((2 * h + 1, 3, U)), dma((2 * h + 1, 3, U)),
        ],
        compiler_params=pltpu.CompilerParams(
            collective_id=0, has_side_effects=True, vmem_limit_bytes=24 * 1024 * 1024),
        name="fused_step",
    )(*args[:6], args[6].reshape(1, S), args[7].reshape(1, S))
    small = jax.ShapeDtypeStruct((1, C), jnp.float32)
    out = pl.pallas_call(
        put_out,
        out_shape=(jax.ShapeDtypeStruct((R * F, C), jnp.bfloat16),) * 2 + (small,) * 2
        + (jax.ShapeDtypeStruct((F * L,), jnp.bfloat16),) + (jax.ShapeDtypeStruct((R, C), jnp.float32),) * 2,
        in_specs=[vmem] * (U + 4),
        out_specs=(anywhere,) * 2 + (vmem,) * 3 + (anywhere,) * 2,
        scratch_shapes=[dma((U + 2,))],
        compiler_params=pltpu.CompilerParams(vmem_limit_bytes=1024 * 1024),
        name="put_out",
    )(*held)
    serving_gate, serving_up, scale_gate, scale_up, serve_norm, whole_gate, whole_up = out
    if L > S * T:
        serve_norm = serve_norm.reshape(F, L)[:, :S * T].reshape(-1)
    return (serving_gate, serving_up, scale_gate.reshape(C), scale_up.reshape(C), serve_norm, whole_gate, whole_up)


def solution(mesh):
    F, T = mesh.shape["fsdp"], mesh.shape["tp"]
    return jax.shard_map(
        functools.partial(per_device, F, T),
        mesh=mesh,
        in_specs=(P("fsdp", "tp"),) * 6 + (P(("fsdp", "tp")),) * 2,
        out_specs=(P(None, "tp"), P(None, "tp"), P("tp"), P("tp"), P(), P("fsdp", "tp"), P("fsdp", "tp")),
        check_vma=False,
    )
```
